32 devices in a mesh: expert: 8 (over z, x), dp: 4 (over y, core).
Axes of the slice: x: 2, y: 2, z: 4, core: 2. Of those that a mesh axis runs over, the one named last changes fastest.
Arguments:
- tokens: bfloat16 [8192, 2048], P(('expert', 'dp')), may hold values from -256 to 256
- routes: int32 [8192, 2], P(('expert', 'dp')), may hold values from 0 to 31, all different within a row
- priority: int32 [32, 256], P(('expert', 'dp')), may hold values from 0 to 255, each once within a row
- router: bfloat16 [2048, 32], replicated, may hold values from -3 to 3
- w_in: bfloat16 [32, 2048, 1024], P(('expert', 'dp')), may hold values from -0.125 to 0.125
- w_out: bfloat16 [32, 2048, 1024], P(('expert', 'dp')), may hold values from -0.1875 to 0.1875
Outputs:
- mixed: bfloat16 [8192, 2048], P(('expert', 'dp'))
- aux_loss: float32 [], replicated
The draws below stay inside these ranges and needn't reach their ends.
Inputs may be any that keep to these rules, and one draw needn't show every extreme that they name: `routes`: a token's two experts differ; every expert is named by some token. `priority`: each group's 256 tokens hold every rank once.
All inputs are finite; a program needn't handle non-finite values.
Results may differ from the reference program's by a relative error of at most 0.0014.
The reference program's roundings to bfloat16 on the way count: a program that leaves them out, or rounds other values in their place, can miss the bound.
Values may be sent and summed in bfloat16 or wider, within the bound.
A program may use at most 64 MiB of HBM per device.

```python
import math
import jax
import jax.numpy as jnp
from jax import lax

D = 2048
FF = 1024
TOK_DEV = 256
EXPERTS = 32
GROUPS = 32
TOKENS = 8192
CAP = 32


def router_values(key):
    sub_key = jax.random.fold_in(key, 71)
    spread = 3.0 / math.sqrt(D)
    values = jnp.clip(jax.random.normal(sub_key, (D, EXPERTS), jnp.float32), -6.0, 6.0) * spread
    return values


def draw_router(key, part):
    return router_values(key).astype(jnp.bfloat16)


def draw_tokens(key, part):
    base = jnp.clip(jax.random.normal(jax.random.fold_in(key, 5), (TOKENS, D), jnp.float32), -6.0, 6.0)
    return base.astype(jnp.bfloat16)


def block_scale(own_key, dims, cuts, low, top_value):
    gain, own = 1.0, jax.random.fold_in(own_key, 6)
    for position, parts in cuts:
        draws = jnp.exp(jax.random.uniform(jax.random.fold_in(own, position), (parts,), jnp.float32, low / len(cuts), top_value / len(cuts)))
        gain = gain * jnp.repeat(draws, dims[position] // parts).reshape([-1 if axis == position else 1 for axis in range(len(dims))])
    return gain


def distinct(rng, rows, count, top, lift):
    sequence = jax.random.permutation(jax.random.fold_in(rng, 1), count)
    favour = sequence
    for power in range(3):
        favour = favour * favour // count
    favour = favour * lift // count
    chance = jax.random.randint(jax.random.fold_in(rng, 2), (rows, count), 0, 4096) + favour
    fixed_rows = jax.random.permutation(jax.random.fold_in(rng, 3), rows)[jnp.arange(count) % rows]
    chance = jnp.where(jnp.arange(rows)[:, None] == fixed_rows[None, :], 1 << 14, chance)
    score = chance * count + jnp.arange(count)
    return lax.top_k(score.astype(jnp.int32), top)[1].astype(jnp.int32)


def noise(key, dims, width, bound, pieces=(), kind=jnp.bfloat16):
    level = block_scale(key, dims, pieces, -0.22, 0.18) if pieces else 1.0
    entries = jax.random.normal(key, dims, jnp.float32) * width * level
    return jnp.minimum(jnp.maximum(entries, -bound), bound).astype(kind)


def setup_inputs(seed: int = 0) -> dict:
    arg_keys = jax.random.split(jax.random.key(seed), 7)
    return {
        "tokens": draw_tokens(jax.random.fold_in(arg_keys[6], 71), 0),
        "routes": distinct(arg_keys[1], TOKENS, EXPERTS, 2, 512),
        "priority": jax.vmap(lambda own: jax.random.permutation(own, TOK_DEV))(jax.random.split(arg_keys[2], GROUPS)).reshape((GROUPS, TOK_DEV)).astype(jnp.int32),
        "router": draw_router(jax.random.fold_in(arg_keys[6], 71), 0),
        "w_in": noise(arg_keys[4], (EXPERTS, D, FF), D ** -0.5, 0.125, ((0, 32),)),
        "w_out": noise(arg_keys[5], (EXPERTS, D, FF), FF ** -0.5, 0.1875, ((0, 32),)),
    }


def reference(tokens, routes, priority, router, w_in, w_out):
    group_count = TOKENS // TOK_DEV
    logits = jnp.dot(tokens, router, preferred_element_type=jnp.float32)
    probs = jax.nn.softmax(logits, axis=-1)
    first = routes[:, 0].astype(jnp.int32)
    second = routes[:, 1].astype(jnp.int32)
    logit_first = jnp.take_along_axis(logits, first[:, None], axis=1)[:, 0]
    logit_second = jnp.take_along_axis(logits, second[:, None], axis=1)[:, 0]
    gate_first = jax.nn.sigmoid(logit_first - logit_second).astype(jnp.bfloat16)
    gate_second = jax.nn.sigmoid(logit_second - logit_first).astype(jnp.bfloat16)
    expert_ids = jnp.arange(EXPERTS, dtype=jnp.int32)
    first_grouped = first.reshape(group_count, TOK_DEV)
    second_grouped = second.reshape(group_count, TOK_DEV)

    def positions(items):
        first_row, second_row, ranks = items
        first_hot = (first_row[:, None] == expert_ids[None, :]).astype(jnp.float32)
        second_hot = (second_row[:, None] == expert_ids[None, :]).astype(jnp.float32)
        earlier = (ranks[None, :] < ranks[:, None]).astype(jnp.float32)
        before_first = jnp.dot(earlier, first_hot, preferred_element_type=jnp.float32)
        before_second = jnp.dot(earlier, second_hot, preferred_element_type=jnp.float32)
        first_load = jnp.sum(first_hot, axis=0)
        pos_first = jnp.sum(before_first * first_hot, axis=1)
        pos_second = jnp.sum((before_second + first_load[None, :]) * second_hot, axis=1)
        return pos_first.astype(jnp.int32), pos_second.astype(jnp.int32)

    pos_first, pos_second = lax.map(positions, (first_grouped, second_grouped, priority))
    dump_slot = CAP * EXPERTS
    slot_first = jnp.where(pos_first < CAP, pos_first * EXPERTS + first_grouped, dump_slot).astype(jnp.int32)
    slot_second = jnp.where(pos_second < CAP, pos_second * EXPERTS + second_grouped, dump_slot).astype(jnp.int32)
    grouped_tokens = tokens.reshape(group_count, TOK_DEV, D)

    def fill(items):
        rows, first_slots, second_slots = items
        buffer = jnp.zeros((dump_slot + 1, D), jnp.bfloat16)
        buffer = buffer.at[first_slots].set(rows).at[second_slots].set(rows)
        return buffer[:dump_slot]

    buffers = lax.map(fill, (grouped_tokens, slot_first, slot_second))
    by_expert = buffers.reshape(group_count, CAP, EXPERTS, D).transpose(2, 0, 1, 3).reshape(EXPERTS, group_count * CAP, D)

    def expert_ffn(items):
        rows, weight_in, weight_out = items
        hidden = jax.nn.relu(jnp.dot(rows, weight_in, preferred_element_type=jnp.float32)).astype(jnp.bfloat16)
        return jnp.dot(hidden, weight_out.T, preferred_element_type=jnp.float32).astype(jnp.bfloat16)

    produced = lax.map(expert_ffn, (by_expert, w_in, w_out))
    returned = produced.reshape(EXPERTS, group_count, CAP, D).transpose(1, 2, 0, 3).reshape(group_count, dump_slot, D)
    returned = jnp.concatenate([returned, jnp.zeros((group_count, 1, D), jnp.bfloat16)], axis=1)

    def combine(items):
        table, first_slots, second_slots, weight_first, weight_second = items
        rows_first = table[first_slots].astype(jnp.float32)
        rows_second = table[second_slots].astype(jnp.float32)
        total = weight_first.astype(jnp.float32)[:, None] * rows_first + weight_second.astype(jnp.float32)[:, None] * rows_second
        return total.astype(jnp.bfloat16)

    mixed = lax.map(combine, (returned, slot_first, slot_second, gate_first.reshape(group_count, TOK_DEV), gate_second.reshape(group_count, TOK_DEV)))
    mixed = mixed.reshape(TOKENS, D)
    mean_prob = jnp.mean(probs, axis=0)
    first_share = jnp.mean((first[:, None] == expert_ids[None, :]).astype(jnp.float32), axis=0)
    aux_loss = EXPERTS * jnp.sum(mean_prob * first_share)
    return mixed, aux_loss
```

```python
import functools

import jax
import jax.numpy as jnp
from jax import lax
from jax.experimental import pallas as pl
from jax.experimental.pallas import tpu as pltpu
from jax.sharding import PartitionSpec as P

MESH = pl.DeviceIdType.MESH
LINES = 4


def exchange_kernel(
    lanes,
    columns,
    cap,
    tokens,
    meta,
    combine,
    stats,
    w_in_hbm,
    w_out_hbm,
    mixed,
    aux,
    tok_all,
    meta_all,
    out,
    arrived,
    produced,
    returned,
    hidden,
    total,
    stats_all,
    w_in,
    w_out,
    weight_sem,
    tok_send,
    tok_recv,
    meta_send,
    meta_recv,
    stat_send,
    stat_recv,
    out_send,
    out_recv,
    ret_send,
    ret_recv,
):
    plane = lanes * columns
    devices = LINES * plane
    rows = plane * cap
    group_rows, width = tokens.shape
    units = w_in.shape[1]
    owner = lax.axis_index("expert")
    column = lax.axis_index("dp")
    z = owner // lanes
    p = (owner % lanes) * columns + column
    me = z * plane + p

    def place(line, spot):
        return (line * lanes + spot // columns, spot % columns)

    load_in = pltpu.make_async_copy(w_in_hbm.at[0], w_in, weight_sem.at[0])
    load_out = pltpu.make_async_copy(w_out_hbm.at[0], w_out, weight_sem.at[1])
    load_in.start()
    load_out.start()

    barrier = pltpu.get_barrier_semaphore()
    for shift in range(1, devices):
        other = (me + shift) % devices
        pl.semaphore_signal(
            barrier, inc=1, device_id=place(other // plane, other % plane), device_id_type=MESH
        )
    pl.semaphore_wait(barrier, devices - 1)

    def line_copies(group, own, way):
        line = z + 1 - 2 * way
        return (
            pltpu.make_async_remote_copy(
                src_ref=meta if own else meta_all.at[group],
                dst_ref=meta_all.at[group],
                send_sem=meta_send.at[way, group],
                recv_sem=meta_recv.at[group],
                device_id=place(line, p),
                device_id_type=MESH,
            ),
            pltpu.make_async_remote_copy(
                src_ref=tokens if own else tok_all.at[group],
                dst_ref=tok_all.at[group],
                send_sem=tok_send.at[way, group],
                recv_sem=tok_recv.at[group],
                device_id=place(line, p),
                device_id_type=MESH,
            ),
        )

    def send_line(group, own, way):
        for copy in line_copies(group, own, way):
            copy.start()

    def take_line(group):
        for copy in line_copies(group, False, 0):
            copy.wait_recv()

    @pl.when(z < LINES - 1)
    def _():
        send_line(z, True, 0)

    @pl.when(z > 0)
    def _():
        send_line(z, True, 1)

    def stat_copy(shift):
        other = (me + shift) % devices
        return pltpu.make_async_remote_copy(
            src_ref=stats,
            dst_ref=stats_all.at[shift],
            send_sem=stat_send.at[shift],
            recv_sem=stat_recv.at[shift],
            device_id=place(other // plane, other % plane),
            device_id_type=MESH,
        )

    for shift in range(1, devices):
        stat_copy(shift).start()

    half = z // (LINES // 2)
    near = z * (1 - half) + (LINES - 1 - z) * half
    order = []
    for value in (near, 1 + near, 2 - 2 * near, LINES - 1):
        order.append(value * (1 - half) + (LINES - 1 - value) * half)

    def hop(distance):
        @pl.when(z >= distance)
        def _():
            take_line(z - distance)

            @pl.when(z < LINES - 1)
            def _():
                send_line(z - distance, False, 0)

        @pl.when(z + distance < LINES)
        def _():
            take_line(z + distance)

            @pl.when(z > 0)
            def _():
                send_line(z + distance, False, 1)

    def out_copy(step, shift):
        spot = (p + shift) % plane
        return pltpu.make_async_remote_copy(
            src_ref=out.at[step, pl.ds(pl.multiple_of(spot * cap, cap), cap)],
            dst_ref=arrived.at[step, pl.ds(pl.multiple_of(p * cap, cap), cap)],
            send_sem=out_send.at[step, shift],
            recv_sem=out_recv.at[step, shift],
            device_id=place(z, spot),
            device_id_type=MESH,
        )

    def own_out(step):
        mine = pl.ds(pl.multiple_of(p * cap, cap), cap)
        return pltpu.make_async_copy(
            out.at[step, mine], arrived.at[step, mine], out_recv.at[step, 0]
        )

    def dispatch(step):
        group = order[step]
        slots = (meta if step == 0 else meta_all.at[group])[...] - z * rows
        grid = lax.broadcasted_iota(jnp.int32, (rows, group_rows), 0)
        hot = (grid == slots[0:1, :]) | (grid == slots[1:2, :])
        hot = jnp.where(hot, 1.0, 0.0).astype(jnp.bfloat16)
        tile = 512

        def body(j, carry):
            cols = pl.ds(pl.multiple_of(j * tile, tile), tile)
            block = tokens[:, cols] if step == 0 else tok_all[group, :, cols]
            out[step, :, cols] = jnp.dot(
                hot, block, preferred_element_type=jnp.float32
            ).astype(jnp.bfloat16)
            return carry

        lax.fori_loop(0, width // tile, body, 0)
        own_out(step).start()
        for shift in range(1, plane):
            out_copy(step, shift).start()

    def ret_copy(step, shift):
        spot = (p + shift) % plane
        return pltpu.make_async_remote_copy(
            src_ref=produced.at[step, pl.ds(pl.multiple_of(spot * cap, cap), cap)],
            dst_ref=returned.at[z, pl.ds(pl.multiple_of(p * cap, cap), cap)],
            send_sem=ret_send.at[step, shift],
            recv_sem=ret_recv.at[z, shift],
            device_id=place(order[step], spot),
            device_id_type=MESH,
        )

    def own_ret():
        mine = pl.ds(pl.multiple_of(p * cap, cap), cap)
        return pltpu.make_async_copy(
            produced.at[0, mine], returned.at[z, mine], ret_recv.at[z, 0]
        )

    def run_expert(step):
        own_out(step).wait()
        for shift in range(1, plane):
            out_copy(step, shift).wait_recv()
        if step == 0:
            load_in.wait()
            load_out.wait()
        tile = 256

        def up(j, carry):
            cols = pl.ds(pl.multiple_of(j * tile, tile), tile)
            value = jnp.dot(arrived[step], w_in[:, cols], preferred_element_type=jnp.float32)
            hidden[:, cols] = jnp.maximum(value, 0.0).astype(jnp.bfloat16)
            return carry

        lax.fori_loop(0, units // tile, up, 0)

        def down(j, carry):
            cols = pl.ds(pl.multiple_of(j * tile, tile), tile)
            value = lax.dot_general(
                hidden[...],
                w_out[cols, :],
                (((1,), (1,)), ((), ())),
                preferred_element_type=jnp.float32,
            )
            produced[step, :, cols] = value.astype(jnp.bfloat16)
            return carry

        lax.fori_loop(0, width // tile, down, 0)
        if step == 0:
            own_ret().start()
        for shift in range(1 if step == 0 else 0, plane):
            ret_copy(step, shift).start()

    def gather(step):
        line = order[step]
        if step == 0:
            own_ret().wait()
        for shift in range(1 if step == 0 else 0, plane):
            pltpu.make_async_remote_copy(
                src_ref=produced.at[0, pl.ds(0, cap)],
                dst_ref=returned.at[line, pl.ds(pl.multiple_of(((p + plane - shift) % plane) * cap, cap), cap)],
                send_sem=ret_send.at[0, shift],
                recv_sem=ret_recv.at[line, shift],
                device_id=place(line, p),
                device_id_type=MESH,
            ).wait_recv()
        tile = 512

        def body(j, carry):
            cols = pl.ds(pl.multiple_of(j * tile, tile), tile)
            value = jnp.dot(
                combine[line], returned[line, :, cols], preferred_element_type=jnp.float32
            )
            if step > 0:
                value = total[:, cols] + value
            if step < LINES - 1:
                total[:, cols] = value
            else:
                mixed[:, cols] = value.astype(jnp.bfloat16)
            return carry

        lax.fori_loop(0, width // tile, body, 0)

    dispatch(0)
    run_expert(0)
    hop(1)
    dispatch(1)
    run_expert(1)
    hop(2)
    dispatch(2)
    run_expert(2)
    hop(3)
    dispatch(3)
    run_expert(3)
    gather(0)

    sums = stats[...]
    for shift in range(1, devices):
        stat_copy(shift).wait()
        sums = sums + stats_all[shift]
    everyone = group_rows * devices
    share = (sums[0:1, :] / everyone) * (sums[1:2, :] / everyone)
    aux[...] = jnp.broadcast_to(devices * jnp.sum(share, axis=1, keepdims=True), aux.shape)

    gather(1)
    gather(2)
    gather(3)

    for way in range(2):
        moves = (z < LINES - 1) if way == 0 else (z > 0)

        @pl.when(moves)
        def _():
            for copy in line_copies(z, True, way):
                copy.wait_send()

        for distance in range(1, LINES):
            passes = (z >= distance) if way == 0 else (z + distance < LINES)

            @pl.when(moves & passes)
            def _():
                group = z - distance if way == 0 else z + distance
                for copy in line_copies(group, False, way):
                    copy.wait_send()

    for step in range(LINES):
        for shift in range(1, plane):
            out_copy(step, shift).wait_send()
        for shift in range(1 if step == 0 else 0, plane):
            ret_copy(step, shift).wait_send()


def exchange(tokens, meta, combine, stats, w_in, w_out, lanes, columns, cap):
    group_rows, width = tokens.shape
    units = w_in.shape[2]
    plane = lanes * columns
    rows = plane * cap
    devices = LINES * plane
    vmem = pl.BlockSpec(memory_space=pltpu.VMEM)
    anywhere = pl.BlockSpec(memory_space=pl.ANY)
    dma = pltpu.SemaphoreType.DMA
    half = jnp.bfloat16
    return pl.pallas_call(
        functools.partial(exchange_kernel, lanes, columns, cap),
        out_shape=(
            jax.ShapeDtypeStruct((group_rows, width), half),
            jax.ShapeDtypeStruct((8, 128), jnp.float32),
        ),
        in_specs=[vmem, vmem, vmem, vmem, anywhere, anywhere],
        out_specs=(vmem, vmem),
        scratch_shapes=[
            pltpu.VMEM((LINES, group_rows, width), half),
            pltpu.VMEM((LINES,) + meta.shape, jnp.int32),
            pltpu.VMEM((LINES, rows, width), half),
            pltpu.VMEM((LINES, rows, width), half),
            pltpu.VMEM((LINES, rows, width), half),
            pltpu.VMEM((LINES, rows, width), half),
            pltpu.VMEM((rows, units), half),
            pltpu.VMEM((group_rows, width), jnp.float32),
            pltpu.VMEM((devices,) + stats.shape, jnp.float32),
            pltpu.VMEM((width, units), half),
            pltpu.VMEM((width, units), half),
            dma((2,)),
            dma((2, LINES)),
            dma((LINES,)),
            dma((2, LINES)),
            dma((LINES,)),
            dma((devices,)),
            dma((devices,)),
            dma((LINES, plane)),
            dma((LINES, plane)),
            dma((LINES, plane)),
            dma((LINES, plane)),
        ],
        compiler_params=pltpu.CompilerParams(
            collective_id=0, has_side_effects=True, vmem_limit_bytes=60 * 1024 * 1024
        ),
    )(tokens, meta, combine, stats, w_in, w_out)


def send_rows(outgoing):
    column = lax.all_to_all(outgoing, "dp", split_axis=1, concat_axis=1, tiled=True)
    arrived = lax.all_to_all(column, "expert", split_axis=0, concat_axis=0, tiled=True)
    return arrived


def return_rows(produced):
    column = lax.all_to_all(produced, "expert", split_axis=0, concat_axis=0, tiled=True)
    returned = lax.all_to_all(column, "dp", split_axis=1, concat_axis=1, tiled=True)
    return returned


def shards(tokens, routes, priority, router, w_in, w_out):
    group_rows = tokens.shape[0]
    width = tokens.shape[1]
    experts = router.shape[1]
    slot_cap = 4 * group_rows // experts
    owner_count = lax.axis_size("expert")
    column_count = lax.axis_size("dp")
    logits = jnp.dot(tokens, router, preferred_element_type=jnp.float32)
    probs = jax.nn.softmax(logits, axis=-1)
    expert_grid = lax.broadcasted_iota(jnp.int32, (group_rows, experts), 1)
    first = routes[:, 0]
    second = routes[:, 1]
    first_hot = (expert_grid == first[:, None]).astype(jnp.float32)
    second_hot = (expert_grid == second[:, None]).astype(jnp.float32)
    logit_first = jnp.sum(logits * first_hot, axis=1)
    logit_second = jnp.sum(logits * second_hot, axis=1)
    gate_first = jax.nn.sigmoid(logit_first - logit_second).astype(jnp.bfloat16)
    gate_second = jax.nn.sigmoid(logit_second - logit_first).astype(jnp.bfloat16)
    ranks = priority[0]
    earlier = (ranks[None, :] < ranks[:, None]).astype(jnp.bfloat16)
    before_first = jnp.dot(
        earlier, first_hot.astype(jnp.bfloat16), preferred_element_type=jnp.float32
    )
    before_second = jnp.dot(
        earlier, second_hot.astype(jnp.bfloat16), preferred_element_type=jnp.float32
    )
    first_load = jnp.sum(first_hot, axis=0)
    pos_first = jnp.sum(before_first * first_hot, axis=1).astype(jnp.int32)
    pos_second = jnp.sum((before_second + first_load[None, :]) * second_hot, axis=1).astype(
        jnp.int32
    )
    slot_first = jnp.where(pos_first < slot_cap, first * slot_cap + pos_first, -1)
    slot_second = jnp.where(pos_second < slot_cap, second * slot_cap + pos_second, -1)
    prob_sum = jnp.sum(probs, axis=0)
    if owner_count % LINES == 0 and slot_cap % 16 == 0:
        lanes = owner_count // LINES
        rows = lanes * column_count * slot_cap
        whole_grid = (LINES, group_rows, rows)
        seats = lax.broadcasted_iota(jnp.int32, whole_grid, 0) * rows + lax.broadcasted_iota(
            jnp.int32, whole_grid, 2
        )
        nothing = jnp.zeros((), jnp.bfloat16)
        combine = jnp.where(
            seats == slot_first[None, :, None], gate_first[None, :, None], nothing
        ) + jnp.where(seats == slot_second[None, :, None], gate_second[None, :, None], nothing)
        meta = jnp.pad(jnp.stack([slot_first, slot_second], axis=0), ((0, 6), (0, 0)))
        statistics = jnp.stack([prob_sum, first_load], axis=0)
        statistics = jnp.pad(statistics, ((0, 6), (0, -experts % 128)))
        mixed, aux = exchange(
            tokens, meta, combine, statistics, w_in, w_out, lanes, column_count, slot_cap
        )
        return (mixed, aux[0, 0])
    slot_grid = lax.broadcasted_iota(jnp.int32, (experts * slot_cap, group_rows), 0)
    dispatch = ((slot_grid == slot_first[None, :]) | (slot_grid == slot_second[None, :])).astype(
        jnp.bfloat16
    )
    outgoing = jnp.dot(dispatch, tokens, preferred_element_type=jnp.float32).astype(jnp.bfloat16)
    outgoing = outgoing.reshape(owner_count, column_count, slot_cap, width)
    arrived = send_rows(outgoing)
    expert_rows = arrived.reshape(experts * slot_cap, width)
    hidden = jax.nn.relu(jnp.dot(expert_rows, w_in[0], preferred_element_type=jnp.float32)).astype(
        jnp.bfloat16
    )
    produced = lax.dot_general(
        hidden, w_out[0], (((1,), (1,)), ((), ())), preferred_element_type=jnp.float32
    ).astype(jnp.bfloat16)
    returned = return_rows(produced.reshape(owner_count, column_count, slot_cap, width))
    returned = returned.reshape(experts * slot_cap, width)
    token_grid = lax.broadcasted_iota(jnp.int32, (group_rows, experts * slot_cap), 1)
    nothing = jnp.zeros((), jnp.bfloat16)
    combine = jnp.where(
        token_grid == slot_first[:, None], gate_first[:, None], nothing
    ) + jnp.where(token_grid == slot_second[:, None], gate_second[:, None], nothing)
    mixed = jnp.dot(combine, returned, preferred_element_type=jnp.float32).astype(jnp.bfloat16)
    statistics = jnp.stack([prob_sum, first_load], axis=0)
    all_tokens = group_rows * owner_count * column_count
    totals = lax.psum(statistics, ("expert", "dp"))
    aux_loss = experts * jnp.sum(totals[0] / all_tokens * (totals[1] / all_tokens))
    return (mixed, aux_loss)


def solution(mesh):
    placed = (
        P(("expert", "dp"), None),
        P(("expert", "dp"), None),
        P(("expert", "dp"), None),
        P(),
        P(("expert", "dp"), None, None),
        P(("expert", "dp"), None, None),
    )
    return jax.shard_map(
        shards,
        mesh=mesh,
        in_specs=placed,
        out_specs=(P(("expert", "dp"), None), P()),
        check_vma=False,
    )
```

```python
import functools

import jax
import jax.numpy as jnp
from jax import lax
from jax.experimental import pallas as pl
from jax.experimental.pallas import tpu as pltpu
from jax.sharding import PartitionSpec as P

MESH = pl.DeviceIdType.MESH
LINES = 4


def route(tokens, routes, priority, router, meta, gates, stats, cap):
    experts = router.shape[0]
    group_rows = tokens.shape[0]
    logits = lax.dot_general(
        router[...], tokens[...], (((1,), (1,)), ((), ())), preferred_element_type=jnp.float32
    )
    shifted = jnp.exp(logits - jnp.max(logits, axis=0, keepdims=True))
    probs = shifted / jnp.sum(shifted, axis=0, keepdims=True)
    grid = lax.broadcasted_iota(jnp.int32, (experts, group_rows), 0)
    first = routes[0:1, :]
    second = routes[1:2, :]
    first_hot = jnp.where(grid == first, 1.0, 0.0)
    second_hot = jnp.where(grid == second, 1.0, 0.0)
    margin = jnp.sum(logits * first_hot, axis=0, keepdims=True) - jnp.sum(
        logits * second_hot, axis=0, keepdims=True
    )
    gate_first = (1.0 / (1.0 + jnp.exp(-margin))).astype(jnp.bfloat16).astype(jnp.float32)
    gate_second = (1.0 / (1.0 + jnp.exp(margin))).astype(jnp.bfloat16).astype(jnp.float32)
    ranks = jnp.broadcast_to(priority[0:1, :].astype(jnp.float32), (group_rows, group_rows))
    earlier = jnp.where(jnp.transpose(ranks) < ranks, 1.0, 0.0).astype(jnp.bfloat16)
    before_first = jnp.dot(
        first_hot.astype(jnp.bfloat16), earlier, preferred_element_type=jnp.float32
    )
    before_second = jnp.dot(
        second_hot.astype(jnp.bfloat16), earlier, preferred_element_type=jnp.float32
    )
    load = jnp.sum(first_hot, axis=1, keepdims=True)
    pos_first = jnp.sum(before_first * first_hot, axis=0, keepdims=True).astype(jnp.int32)
    pos_second = jnp.sum((before_second + load) * second_hot, axis=0, keepdims=True).astype(
        jnp.int32
    )
    meta[...] = jnp.full(meta.shape, -1, jnp.int32)
    meta[0:1, :] = jnp.where(pos_first < cap, first * cap + pos_first, -1)
    meta[1:2, :] = jnp.where(pos_second < cap, second * cap + pos_second, -1)
    gates[0:1, :] = gate_first
    gates[1:2, :] = gate_second
    ones = jnp.ones((8, group_rows), jnp.float32)
    sums = []
    for table in (probs, first_hot):
        sums.append(
            lax.dot_general(
                ones,
                table,
                (((1,), (1,)), ((), ())),
                precision=lax.Precision.HIGHEST,
                preferred_element_type=jnp.float32,
            )
        )
    row = lax.broadcasted_iota(jnp.int32, sums[0].shape, 0)
    stats[...] = jnp.where(row == 0, sums[0], sums[1])


def exchange_kernel(
    lanes,
    columns,
    cap,
    tokens,
    routes,
    priority,
    router,
    w_in_hbm,
    w_out_hbm,
    mixed,
    aux,
    meta,
    gates,
    stats,
    tok_all,
    meta_all,
    out,
    arrived,
    produced,
    returned,
    hidden,
    total,
    stats_all,
    w_in,
    w_out,
    weight_sem,
    tok_send,
    tok_recv,
    meta_send,
    meta_recv,
    stat_send,
    stat_recv,
    out_send,
    out_recv,
    ret_send,
    ret_recv,
):
    plane = lanes * columns
    devices = LINES * plane
    rows = plane * cap
    group_rows, width = tokens.shape
    units = w_in.shape[1]
    owner = lax.axis_index("expert")
    column = lax.axis_index("dp")
    z = owner // lanes
    p = (owner % lanes) * columns + column
    me = z * plane + p

    def place(line, spot):
        return (line * lanes + spot // columns, spot % columns)

    load_in = pltpu.make_async_copy(w_in_hbm.at[0], w_in, weight_sem.at[0])
    load_out = pltpu.make_async_copy(w_out_hbm.at[0], w_out, weight_sem.at[1])
    load_in.start()
    load_out.start()

    barrier = pltpu.get_barrier_semaphore()
    for shift in range(1, devices):
        other = (me + shift) % devices
        pl.semaphore_signal(
            barrier, inc=1, device_id=place(other // plane, other % plane), device_id_type=MESH
        )
    pl.semaphore_wait(barrier, devices - 1)

    def line_copies(group, own, way):
        line = z + 1 - 2 * way
        return (
            pltpu.make_async_remote_copy(
                src_ref=meta if own else meta_all.at[group],
                dst_ref=meta_all.at[group],
                send_sem=meta_send.at[way, group],
                recv_sem=meta_recv.at[group],
                device_id=place(line, p),
                device_id_type=MESH,
            ),
            pltpu.make_async_remote_copy(
                src_ref=tokens if own else tok_all.at[group],
                dst_ref=tok_all.at[group],
                send_sem=tok_send.at[way, group],
                recv_sem=tok_recv.at[group],
                device_id=place(line, p),
                device_id_type=MESH,
            ),
        )

    def send_line(group, own, way, parts=(0, 1)):
        copies = line_copies(group, own, way)
        for part in parts:
            copies[part].start()

    def take_line(group):
        for copy in line_copies(group, False, 0):
            copy.wait_recv()

    def send_own(parts):
        @pl.when(z < LINES - 1)
        def _():
            send_line(z, True, 0, parts)

        @pl.when(z > 0)
        def _():
            send_line(z, True, 1, parts)

    send_own((1,))
    route(tokens, routes, priority, router, meta, gates, stats, cap)

    def stat_copy(shift):
        other = (me + shift) % devices
        return pltpu.make_async_remote_copy(
            src_ref=stats,
            dst_ref=stats_all.at[shift],
            send_sem=stat_send.at[shift],
            recv_sem=stat_recv.at[shift],
            device_id=place(other // plane, other % plane),
            device_id_type=MESH,
        )

    half = z // (LINES // 2)
    near = z * (1 - half) + (LINES - 1 - z) * half
    order = []
    for value in (near, 1 + near, 2 + near, 3 - 3 * near):
        order.append(value * (1 - half) + (LINES - 1 - value) * half)

    def hop(distance):
        @pl.when(z >= distance)
        def _():
            take_line(z - distance)

            @pl.when(z < LINES - 1)
            def _():
                send_line(z - distance, False, 0)

        @pl.when(z + distance < LINES)
        def _():
            take_line(z + distance)

            @pl.when(z > 0)
            def _():
                send_line(z + distance, False, 1)

    def out_copy(step, shift):
        spot = (p + shift) % plane
        return pltpu.make_async_remote_copy(
            src_ref=out.at[step, pl.ds(pl.multiple_of(spot * cap, cap), cap)],
            dst_ref=arrived.at[step, pl.ds(pl.multiple_of(p * cap, cap), cap)],
            send_sem=out_send.at[step, shift],
            recv_sem=out_recv.at[step, shift],
            device_id=place(z, spot),
            device_id_type=MESH,
        )

    def own_out(step):
        mine = pl.ds(pl.multiple_of(p * cap, cap), cap)
        return pltpu.make_async_copy(
            out.at[step, mine], arrived.at[step, mine], out_recv.at[step, 0]
        )

    def dispatch(step):
        group = order[step]
        slots = (meta if step == 0 else meta_all.at[group])[...] - z * rows
        grid = lax.broadcasted_iota(jnp.int32, (rows, group_rows), 0)
        hot = (grid == slots[0:1, :]) | (grid == slots[1:2, :])
        hot = jnp.where(hot, 1.0, 0.0).astype(jnp.bfloat16)
        tile = 512

        def body(j, carry):
            cols = pl.ds(pl.multiple_of(j * tile, tile), tile)
            block = tokens[:, cols] if step == 0 else tok_all[group, :, cols]
            out[step, :, cols] = jnp.dot(
                hot, block, preferred_element_type=jnp.float32
            ).astype(jnp.bfloat16)
            return carry

        lax.fori_loop(0, width // tile, body, 0)
        own_out(step).start()
        for shift in range(1, plane):
            out_copy(step, shift).start()

    def ret_copy(step, shift):
        spot = (p + shift) % plane
        return pltpu.make_async_remote_copy(
            src_ref=produced.at[step, pl.ds(pl.multiple_of(spot * cap, cap), cap)],
            dst_ref=returned.at[z, pl.ds(pl.multiple_of(p * cap, cap), cap)],
            send_sem=ret_send.at[step, shift],
            recv_sem=ret_recv.at[z, shift],
            device_id=place(order[step], spot),
            device_id_type=MESH,
        )

    def own_ret():
        mine = pl.ds(pl.multiple_of(p * cap, cap), cap)
        return pltpu.make_async_copy(
            produced.at[0, mine], returned.at[z, mine], ret_recv.at[z, 0]
        )

    def run_expert(step):
        own_out(step).wait()
        for shift in range(1, plane):
            out_copy(step, shift).wait_recv()
        if step == 0:
            load_in.wait()
            load_out.wait()
        tile = 256

        def up(j, carry):
            cols = pl.ds(pl.multiple_of(j * tile, tile), tile)
            value = jnp.dot(arrived[step], w_in[:, cols], preferred_element_type=jnp.float32)
            hidden[:, cols] = jnp.maximum(value, 0.0).astype(jnp.bfloat16)
            return carry

        lax.fori_loop(0, units // tile, up, 0)

        def down(j, carry):
            cols = pl.ds(pl.multiple_of(j * tile, tile), tile)
            value = lax.dot_general(
                hidden[...],
                w_out[cols, :],
                (((1,), (1,)), ((), ())),
                preferred_element_type=jnp.float32,
            )
            produced[step, :, cols] = value.astype(jnp.bfloat16)
            return carry

        lax.fori_loop(0, width // tile, down, 0)
        if step == 0:
            own_ret().start()
        for shift in range(1 if step == 0 else 0, plane):
            ret_copy(step, shift).start()

    def gather(step):
        line = order[step]
        if step == 0:
            own_ret().wait()
        for shift in range(1 if step == 0 else 0, plane):
            pltpu.make_async_remote_copy(
                src_ref=produced.at[0, pl.ds(0, cap)],
                dst_ref=returned.at[line, pl.ds(pl.multiple_of(((p + plane - shift) % plane) * cap, cap), cap)],
                send_sem=ret_send.at[0, shift],
                recv_sem=ret_recv.at[line, shift],
                device_id=place(line, p),
                device_id_type=MESH,
            ).wait_recv()
        tile = 512
        grid = lax.broadcasted_iota(jnp.int32, (rows, group_rows), 0) + line * rows
        weights = jnp.where(grid == meta[0:1, :], gates[0:1, :], 0.0)
        weights = weights + jnp.where(grid == meta[1:2, :], gates[1:2, :], 0.0)
        weights = jnp.transpose(weights).astype(jnp.bfloat16)

        def body(j, carry):
            cols = pl.ds(pl.multiple_of(j * tile, tile), tile)
            value = jnp.dot(
                weights, returned[line, :, cols], preferred_element_type=jnp.float32
            )
            if step > 0:
                value = total[:, cols] + value
            if step < LINES - 1:
                total[:, cols] = value
            else:
                mixed[:, cols] = value.astype(jnp.bfloat16)
            return carry

        lax.fori_loop(0, width // tile, body, 0)

    dispatch(0)
    send_own((0,))
    for shift in range(1, devices):
        stat_copy(shift).start()
    run_expert(0)
    hop(1)
    dispatch(1)
    run_expert(1)
    hop(2)
    dispatch(2)
    run_expert(2)
    hop(3)
    dispatch(3)
    run_expert(3)
    gather(0)

    sums = stats[...]
    for shift in range(1, devices):
        stat_copy(shift).wait()
        sums = sums + stats_all[shift]
    everyone = group_rows * devices
    share = (sums[0:1, :] / everyone) * (sums[1:2, :] / everyone)
    aux[...] = jnp.broadcast_to(devices * jnp.sum(share, axis=1, keepdims=True), aux.shape)

    gather(1)
    gather(2)
    gather(3)

    for way in range(2):
        moves = (z < LINES - 1) if way == 0 else (z > 0)

        @pl.when(moves)
        def _():
            for copy in line_copies(z, True, way):
                copy.wait_send()

        for distance in range(1, LINES):
            passes = (z >= distance) if way == 0 else (z + distance < LINES)

            @pl.when(moves & passes)
            def _():
                group = z - distance if way == 0 else z + distance
                for copy in line_copies(group, False, way):
                    copy.wait_send()

    for step in range(LINES):
        for shift in range(1, plane):
            out_copy(step, shift).wait_send()
        for shift in range(1 if step == 0 else 0, plane):
            ret_copy(step, shift).wait_send()


def exchange(tokens, routes, priority, router, w_in, w_out, lanes, columns, cap):
    group_rows, width = tokens.shape
    units = w_in.shape[2]
    plane = lanes * columns
    rows = plane * cap
    devices = LINES * plane
    vmem = pl.BlockSpec(memory_space=pltpu.VMEM)
    anywhere = pl.BlockSpec(memory_space=pl.ANY)
    dma = pltpu.SemaphoreType.DMA
    half = jnp.bfloat16
    return pl.pallas_call(
        functools.partial(exchange_kernel, lanes, columns, cap),
        out_shape=(
            jax.ShapeDtypeStruct((group_rows, width), half),
            jax.ShapeDtypeStruct((8, 128), jnp.float32),
        ),
        in_specs=[vmem, vmem, vmem, vmem, anywhere, anywhere],
        out_specs=(vmem, vmem),
        scratch_shapes=[
            pltpu.VMEM((8, group_rows), jnp.int32),
            pltpu.VMEM((8, group_rows), jnp.float32),
            pltpu.VMEM((8, router.shape[0]), jnp.float32),
            pltpu.VMEM((LINES, group_rows, width), half),
            pltpu.VMEM((LINES, 8, group_rows), jnp.int32),
            pltpu.VMEM((LINES, rows, width), half),
            pltpu.VMEM((LINES, rows, width), half),
            pltpu.VMEM((LINES, rows, width), half),
            pltpu.VMEM((LINES, rows, width), half),
            pltpu.VMEM((rows, units), half),
            pltpu.VMEM((group_rows, width), jnp.float32),
            pltpu.VMEM((devices, 8, router.shape[0]), jnp.float32),
            pltpu.VMEM((width, units), half),
            pltpu.VMEM((width, units), half),
            dma((2,)),
            dma((2, LINES)),
            dma((LINES,)),
            dma((2, LINES)),
            dma((LINES,)),
            dma((devices,)),
            dma((devices,)),
            dma((LINES, plane)),
            dma((LINES, plane)),
            dma((LINES, plane)),
            dma((LINES, plane)),
        ],
        compiler_params=pltpu.CompilerParams(
            collective_id=0, has_side_effects=True, vmem_limit_bytes=60 * 1024 * 1024
        ),
    )(tokens, routes, priority, router, w_in, w_out)


def send_rows(outgoing):
    column = lax.all_to_all(outgoing, "dp", split_axis=1, concat_axis=1, tiled=True)
    arrived = lax.all_to_all(column, "expert", split_axis=0, concat_axis=0, tiled=True)
    return arrived


def return_rows(produced):
    column = lax.all_to_all(produced, "expert", split_axis=0, concat_axis=0, tiled=True)
    returned = lax.all_to_all(column, "dp", split_axis=1, concat_axis=1, tiled=True)
    return returned


def shards(tokens, routes, priority, router, w_in, w_out):
    group_rows = tokens.shape[0]
    width = tokens.shape[1]
    experts = router.shape[1]
    slot_cap = 4 * group_rows // experts
    owner_count = lax.axis_size("expert")
    column_count = lax.axis_size("dp")
    if owner_count % LINES == 0 and slot_cap % 16 == 0:
        lanes = owner_count // LINES
        mixed, aux = exchange(
            tokens, routes.T, priority, router.T, w_in, w_out, lanes, column_count, slot_cap
        )
        return (mixed, aux[0, 0])
    logits = jnp.dot(tokens, router, preferred_element_type=jnp.float32)
    probs = jax.nn.softmax(logits, axis=-1)
    expert_grid = lax.broadcasted_iota(jnp.int32, (group_rows, experts), 1)
    first = routes[:, 0]
    second = routes[:, 1]
    first_hot = (expert_grid == first[:, None]).astype(jnp.float32)
    second_hot = (expert_grid == second[:, None]).astype(jnp.float32)
    logit_first = jnp.sum(logits * first_hot, axis=1)
    logit_second = jnp.sum(logits * second_hot, axis=1)
    gate_first = jax.nn.sigmoid(logit_first - logit_second).astype(jnp.bfloat16)
    gate_second = jax.nn.sigmoid(logit_second - logit_first).astype(jnp.bfloat16)
    ranks = priority[0]
    earlier = (ranks[None, :] < ranks[:, None]).astype(jnp.bfloat16)
    before_first = jnp.dot(
        earlier, first_hot.astype(jnp.bfloat16), preferred_element_type=jnp.float32
    )
    before_second = jnp.dot(
        earlier, second_hot.astype(jnp.bfloat16), preferred_element_type=jnp.float32
    )
    first_load = jnp.sum(first_hot, axis=0)
    pos_first = jnp.sum(before_first * first_hot, axis=1).astype(jnp.int32)
    pos_second = jnp.sum((before_second + first_load[None, :]) * second_hot, axis=1).astype(
        jnp.int32
    )
    slot_first = jnp.where(pos_first < slot_cap, first * slot_cap + pos_first, -1)
    slot_second = jnp.where(pos_second < slot_cap, second * slot_cap + pos_second, -1)
    slot_grid = lax.broadcasted_iota(jnp.int32, (experts * slot_cap, group_rows), 0)
    dispatch = ((slot_grid == slot_first[None, :]) | (slot_grid == slot_second[None, :])).astype(
        jnp.bfloat16
    )
    outgoing = jnp.dot(dispatch, tokens, preferred_element_type=jnp.float32).astype(jnp.bfloat16)
    outgoing = outgoing.reshape(owner_count, column_count, slot_cap, width)
    arrived = send_rows(outgoing)
    expert_rows = arrived.reshape(experts * slot_cap, width)
    hidden = jax.nn.relu(jnp.dot(expert_rows, w_in[0], preferred_element_type=jnp.float32)).astype(
        jnp.bfloat16
    )
    produced = lax.dot_general(
        hidden, w_out[0], (((1,), (1,)), ((), ())), preferred_element_type=jnp.float32
    ).astype(jnp.bfloat16)
    returned = return_rows(produced.reshape(owner_count, column_count, slot_cap, width))
    returned = returned.reshape(experts * slot_cap, width)
    token_grid = lax.broadcasted_iota(jnp.int32, (group_rows, experts * slot_cap), 1)
    nothing = jnp.zeros((), jnp.bfloat16)
    combine = jnp.where(
        token_grid == slot_first[:, None], gate_first[:, None], nothing
    ) + jnp.where(token_grid == slot_second[:, None], gate_second[:, None], nothing)
    mixed = jnp.dot(combine, returned, preferred_element_type=jnp.float32).astype(jnp.bfloat16)
    prob_sum = jnp.sum(probs, axis=0)
    statistics = jnp.stack([prob_sum, first_load], axis=0)
    all_tokens = group_rows * owner_count * column_count
    totals = lax.psum(statistics, ("expert", "dp"))
    aux_loss = experts * jnp.sum(totals[0] / all_tokens * (totals[1] / all_tokens))
    return (mixed, aux_loss)


def solution(mesh):
    placed = (
        P(("expert", "dp"), None),
        P(("expert", "dp"), None),
        P(("expert", "dp"), None),
        P(),
        P(("expert", "dp"), None, None),
        P(("expert", "dp"), None, None),
    )
    return jax.shard_map(
        shards,
        mesh=mesh,
        in_specs=placed,
        out_specs=(P(("expert", "dp"), None), P()),
        check_vma=False,
    )
```

```python
import functools

import jax
import jax.numpy as jnp
from jax import lax
from jax.experimental import pallas as pl
from jax.experimental.pallas import tpu as pltpu
from jax.sharding import PartitionSpec as P

MESH = pl.DeviceIdType.MESH
LINES = 4


def route(tokens, routes, priority, router, meta, gates, stats, cap):
    experts = router.shape[0]
    group_rows = tokens.shape[0]
    logits = lax.dot_general(
        router[...], tokens[...], (((1,), (1,)), ((), ())), preferred_element_type=jnp.float32
    )
    shifted = jnp.exp(logits - jnp.max(logits, axis=0, keepdims=True))
    probs = shifted / jnp.sum(shifted, axis=0, keepdims=True)
    grid = lax.broadcasted_iota(jnp.int32, (experts, group_rows), 0)
    first = routes[0:1, :]
    second = routes[1:2, :]
    first_hot = jnp.where(grid == first, 1.0, 0.0)
    second_hot = jnp.where(grid == second, 1.0, 0.0)
    margin = jnp.sum(logits * first_hot, axis=0, keepdims=True) - jnp.sum(
        logits * second_hot, axis=0, keepdims=True
    )
    gate_first = (1.0 / (1.0 + jnp.exp(-margin))).astype(jnp.bfloat16).astype(jnp.float32)
    gate_second = (1.0 / (1.0 + jnp.exp(margin))).astype(jnp.bfloat16).astype(jnp.float32)
    ranks = jnp.broadcast_to(priority[0:1, :].astype(jnp.float32), (group_rows, group_rows))
    earlier = jnp.where(jnp.transpose(ranks) < ranks, 1.0, 0.0).astype(jnp.bfloat16)
    before_first = jnp.dot(
        first_hot.astype(jnp.bfloat16), earlier, preferred_element_type=jnp.float32
    )
    before_second = jnp.dot(
        second_hot.astype(jnp.bfloat16), earlier, preferred_element_type=jnp.float32
    )
    load = jnp.sum(first_hot, axis=1, keepdims=True)
    pos_first = jnp.sum(before_first * first_hot, axis=0, keepdims=True).astype(jnp.int32)
    pos_second = jnp.sum((before_second + load) * second_hot, axis=0, keepdims=True).astype(
        jnp.int32
    )
    meta[...] = jnp.full(meta.shape, -1, jnp.int32)
    meta[0:1, :] = jnp.where(pos_first < cap, first * cap + pos_first, -1)
    meta[1:2, :] = jnp.where(pos_second < cap, second * cap + pos_second, -1)
    gates[0:1, :] = gate_first
    gates[1:2, :] = gate_second
    ones = jnp.ones((8, group_rows), jnp.float32)
    sums = []
    for table in (probs, first_hot):
        sums.append(
            lax.dot_general(
                ones,
                table,
                (((1,), (1,)), ((), ())),
                precision=lax.Precision.HIGHEST,
                preferred_element_type=jnp.float32,
            )
        )
    row = lax.broadcasted_iota(jnp.int32, sums[0].shape, 0)
    stats[...] = jnp.where(row == 0, sums[0], sums[1])


def exchange_kernel(
    lanes,
    columns,
    cap,
    tokens,
    routes,
    priority,
    router,
    w_in_hbm,
    w_out_hbm,
    mixed,
    aux,
    meta,
    gates,
    stats,
    tok_all,
    meta_all,
    out,
    arrived,
    produced,
    returned,
    hidden,
    total,
    stats_all,
    w_in,
    w_out,
    weight_sem,
    tok_send,
    tok_recv,
    meta_send,
    meta_recv,
    stat_send,
    stat_recv,
    out_send,
    out_recv,
    ret_send,
    ret_recv,
):
    plane = lanes * columns
    devices = LINES * plane
    rows = plane * cap
    group_rows, width = tokens.shape
    units = w_in.shape[1]
    owner = lax.axis_index("expert")
    column = lax.axis_index("dp")
    z = owner // lanes
    p = (owner % lanes) * columns + column
    me = z * plane + p

    def place(line, spot):
        return (line * lanes + spot // columns, spot % columns)

    load_in = pltpu.make_async_copy(w_in_hbm.at[0], w_in, weight_sem.at[0])
    load_out = pltpu.make_async_copy(w_out_hbm.at[0], w_out, weight_sem.at[1])
    load_in.start()
    load_out.start()

    barrier = pltpu.get_barrier_semaphore()
    for shift in range(1, devices):
        other = (me + shift) % devices
        pl.semaphore_signal(
            barrier, inc=1, device_id=place(other // plane, other % plane), device_id_type=MESH
        )
    pl.semaphore_wait(barrier, devices - 1)

    def line_copies(group, own, way):
        line = z + 1 - 2 * way
        return (
            pltpu.make_async_remote_copy(
                src_ref=meta if own else meta_all.at[group],
                dst_ref=meta_all.at[group],
                send_sem=meta_send.at[way, group],
                recv_sem=meta_recv.at[group],
                device_id=place(line, p),
                device_id_type=MESH,
            ),
            pltpu.make_async_remote_copy(
                src_ref=tokens if own else tok_all.at[group],
                dst_ref=tok_all.at[group],
                send_sem=tok_send.at[way, group],
                recv_sem=tok_recv.at[group],
                device_id=place(line, p),
                device_id_type=MESH,
            ),
        )

    def send_line(group, own, way, parts=(0, 1)):
        copies = line_copies(group, own, way)
        for part in parts:
            copies[part].start()

    def take_line(group):
        for copy in line_copies(group, False, 0):
            copy.wait_recv()

    def send_own(parts):
        @pl.when(z < LINES - 1)
        def _():
            send_line(z, True, 0, parts)

        @pl.when(z > 0)
        def _():
            send_line(z, True, 1, parts)

    send_own((1,))
    route(tokens, routes, priority, router, meta, gates, stats, cap)

    def stat_copy(shift):
        other = (me + shift) % devices
        return pltpu.make_async_remote_copy(
            src_ref=stats,
            dst_ref=stats_all.at[shift],
            send_sem=stat_send.at[shift],
            recv_sem=stat_recv.at[shift],
            device_id=place(other // plane, other % plane),
            device_id_type=MESH,
        )

    half = z // (LINES // 2)
    near = z * (1 - half) + (LINES - 1 - z) * half
    order = []
    for value in (near, 1 + near, 2 - 2 * near, LINES - 1):
        order.append(value * (1 - half) + (LINES - 1 - value) * half)

    def hop(distance):
        @pl.when(z >= distance)
        def _():
            take_line(z - distance)

            @pl.when(z < LINES - 1)
            def _():
                send_line(z - distance, False, 0)

        @pl.when(z + distance < LINES)
        def _():
            take_line(z + distance)

            @pl.when(z > 0)
            def _():
                send_line(z + distance, False, 1)

    def out_copy(step, shift):
        spot = (p + shift) % plane
        return pltpu.make_async_remote_copy(
            src_ref=out.at[step, pl.ds(pl.multiple_of(spot * cap, cap), cap)],
            dst_ref=arrived.at[step, pl.ds(pl.multiple_of(p * cap, cap), cap)],
            send_sem=out_send.at[step, shift],
            recv_sem=out_recv.at[step, shift],
            device_id=place(z, spot),
            device_id_type=MESH,
        )

    def own_out(step):
        mine = pl.ds(pl.multiple_of(p * cap, cap), cap)
        return pltpu.make_async_copy(
            out.at[step, mine], arrived.at[step, mine], out_recv.at[step, 0]
        )

    def dispatch(step):
        group = order[step]
        slots = (meta if step == 0 else meta_all.at[group])[...] - z * rows
        grid = lax.broadcasted_iota(jnp.int32, (rows, group_rows), 0)
        hot = (grid == slots[0:1, :]) | (grid == slots[1:2, :])
        hot = jnp.where(hot, 1.0, 0.0).astype(jnp.bfloat16)
        tile = 512

        def body(j, carry):
            cols = pl.ds(pl.multiple_of(j * tile, tile), tile)
            block = tokens[:, cols] if step == 0 else tok_all[group, :, cols]
            out[step, :, cols] = jnp.dot(
                hot, block, preferred_element_type=jnp.float32
            ).astype(jnp.bfloat16)
            return carry

        lax.fori_loop(0, width // tile, body, 0)
        own_out(step).start()
        for shift in range(1, plane):
            out_copy(step, shift).start()

    def ret_copy(step, shift):
        spot = (p + shift) % plane
        return pltpu.make_async_remote_copy(
            src_ref=produced.at[step, pl.ds(pl.multiple_of(spot * cap, cap), cap)],
            dst_ref=returned.at[z, pl.ds(pl.multiple_of(p * cap, cap), cap)],
            send_sem=ret_send.at[step, shift],
            recv_sem=ret_recv.at[z, shift],
            device_id=place(order[step], spot),
            device_id_type=MESH,
        )

    def own_ret():
        mine = pl.ds(pl.multiple_of(p * cap, cap), cap)
        return pltpu.make_async_copy(
            produced.at[0, mine], returned.at[z, mine], ret_recv.at[z, 0]
        )

    def run_expert(step):
        own_out(step).wait()
        for shift in range(1, plane):
            out_copy(step, shift).wait_recv()
        if step == 0:
            load_in.wait()
            load_out.wait()
        tile = 256

        def up(j, carry):
            cols = pl.ds(pl.multiple_of(j * tile, tile), tile)
            value = jnp.dot(arrived[step], w_in[:, cols], preferred_element_type=jnp.float32)
            hidden[:, cols] = jnp.maximum(value, 0.0).astype(jnp.bfloat16)
            return carry

        lax.fori_loop(0, units // tile, up, 0)

        def down(j, carry):
            cols = pl.ds(pl.multiple_of(j * tile, tile), tile)
            value = lax.dot_general(
                hidden[...],
                w_out[cols, :],
                (((1,), (1,)), ((), ())),
                preferred_element_type=jnp.float32,
            )
            produced[step, :, cols] = value.astype(jnp.bfloat16)
            return carry

        lax.fori_loop(0, width // tile, down, 0)
        if step == 0:
            own_ret().start()
        for shift in range(1 if step == 0 else 0, plane):
            ret_copy(step, shift).start()

    def gather(step):
        line = order[step]
        if step == 0:
            own_ret().wait()
        for shift in range(1 if step == 0 else 0, plane):
            pltpu.make_async_remote_copy(
                src_ref=produced.at[0, pl.ds(0, cap)],
                dst_ref=returned.at[line, pl.ds(pl.multiple_of(((p + plane - shift) % plane) * cap, cap), cap)],
                send_sem=ret_send.at[0, shift],
                recv_sem=ret_recv.at[line, shift],
                device_id=place(line, p),
                device_id_type=MESH,
            ).wait_recv()
        tile = 512
        grid = lax.broadcasted_iota(jnp.int32, (rows, group_rows), 0) + line * rows
        weights = jnp.where(grid == meta[0:1, :], gates[0:1, :], 0.0)
        weights = weights + jnp.where(grid == meta[1:2, :], gates[1:2, :], 0.0)
        weights = jnp.transpose(weights).astype(jnp.bfloat16)

        def body(j, carry):
            cols = pl.ds(pl.multiple_of(j * tile, tile), tile)
            value = jnp.dot(
                weights, returned[line, :, cols], preferred_element_type=jnp.float32
            )
            if step > 0:
                value = total[:, cols] + value
            if step < LINES - 1:
                total[:, cols] = value
            else:
                mixed[:, cols] = value.astype(jnp.bfloat16)
            return carry

        lax.fori_loop(0, width // tile, body, 0)

    dispatch(0)
    send_own((0,))
    for shift in range(1, devices):
        stat_copy(shift).start()
    run_expert(0)
    hop(1)
    dispatch(1)
    run_expert(1)
    hop(2)
    dispatch(2)
    run_expert(2)
    hop(3)
    dispatch(3)
    run_expert(3)
    gather(0)

    sums = stats[...]
    for shift in range(1, devices):
        stat_copy(shift).wait()
        sums = sums + stats_all[shift]
    everyone = group_rows * devices
    share = (sums[0:1, :] / everyone) * (sums[1:2, :] / everyone)
    aux[...] = jnp.broadcast_to(devices * jnp.sum(share, axis=1, keepdims=True), aux.shape)

    gather(1)
    gather(2)
    gather(3)

    for way in range(2):
        moves = (z < LINES - 1) if way == 0 else (z > 0)

        @pl.when(moves)
        def _():
            for copy in line_copies(z, True, way):
                copy.wait_send()

        for distance in range(1, LINES):
            passes = (z >= distance) if way == 0 else (z + distance < LINES)

            @pl.when(moves & passes)
            def _():
                group = z - distance if way == 0 else z + distance
                for copy in line_copies(group, False, way):
                    copy.wait_send()

    for step in range(LINES):
        for shift in range(1, plane):
            out_copy(step, shift).wait_send()
        for shift in range(1 if step == 0 else 0, plane):
            ret_copy(step, shift).wait_send()


def exchange(tokens, routes, priority, router, w_in, w_out, lanes, columns, cap):
    group_rows, width = tokens.shape
    units = w_in.shape[2]
    plane = lanes * columns
    rows = plane * cap
    devices = LINES * plane
    vmem = pl.BlockSpec(memory_space=pltpu.VMEM)
    anywhere = pl.BlockSpec(memory_space=pl.ANY)
    dma = pltpu.SemaphoreType.DMA
    half = jnp.bfloat16
    return pl.pallas_call(
        functools.partial(exchange_kernel, lanes, columns, cap),
        out_shape=(
            jax.ShapeDtypeStruct((group_rows, width), half),
            jax.ShapeDtypeStruct((8, 128), jnp.float32),
        ),
        in_specs=[vmem, vmem, vmem, vmem, anywhere, anywhere],
        out_specs=(vmem, vmem),
        scratch_shapes=[
            pltpu.VMEM((8, group_rows), jnp.int32),
            pltpu.VMEM((8, group_rows), jnp.float32),
            pltpu.VMEM((8, router.shape[0]), jnp.float32),
            pltpu.VMEM((LINES, group_rows, width), half),
            pltpu.VMEM((LINES, 8, group_rows), jnp.int32),
            pltpu.VMEM((LINES, rows, width), half),
            pltpu.VMEM((LINES, rows, width), half),
            pltpu.VMEM((LINES, rows, width), half),
            pltpu.VMEM((LINES, rows, width), half),
            pltpu.VMEM((rows, units), half),
            pltpu.VMEM((group_rows, width), jnp.float32),
            pltpu.VMEM((devices, 8, router.shape[0]), jnp.float32),
            pltpu.VMEM((width, units), half),
            pltpu.VMEM((width, units), half),
            dma((2,)),
            dma((2, LINES)),
            dma((LINES,)),
            dma((2, LINES)),
            dma((LINES,)),
            dma((devices,)),
            dma((devices,)),
            dma((LINES, plane)),
            dma((LINES, plane)),
            dma((LINES, plane)),
            dma((LINES, plane)),
        ],
        compiler_params=pltpu.CompilerParams(
            collective_id=0, has_side_effects=True, vmem_limit_bytes=60 * 1024 * 1024
        ),
    )(tokens, routes, priority, router, w_in, w_out)


def send_rows(outgoing):
    column = lax.all_to_all(outgoing, "dp", split_axis=1, concat_axis=1, tiled=True)
    arrived = lax.all_to_all(column, "expert", split_axis=0, concat_axis=0, tiled=True)
    return arrived


def return_rows(produced):
    column = lax.all_to_all(produced, "expert", split_axis=0, concat_axis=0, tiled=True)
    returned = lax.all_to_all(column, "dp", split_axis=1, concat_axis=1, tiled=True)
    return returned


def shards(tokens, routes, priority, router, w_in, w_out):
    group_rows = tokens.shape[0]
    width = tokens.shape[1]
    experts = router.shape[1]
    slot_cap = 4 * group_rows // experts
    owner_count = lax.axis_size("expert")
    column_count = lax.axis_size("dp")
    if owner_count % LINES == 0 and slot_cap % 16 == 0:
        lanes = owner_count // LINES
        mixed, aux = exchange(
            tokens, routes.T, priority, router.T, w_in, w_out, lanes, column_count, slot_cap
        )
        return (mixed, aux[0, 0])
    logits = jnp.dot(tokens, router, preferred_element_type=jnp.float32)
    probs = jax.nn.softmax(logits, axis=-1)
    expert_grid = lax.broadcasted_iota(jnp.int32, (group_rows, experts), 1)
    first = routes[:, 0]
    second = routes[:, 1]
    first_hot = (expert_grid == first[:, None]).astype(jnp.float32)
    second_hot = (expert_grid == second[:, None]).astype(jnp.float32)
    logit_first = jnp.sum(logits * first_hot, axis=1)
    logit_second = jnp.sum(logits * second_hot, axis=1)
    gate_first = jax.nn.sigmoid(logit_first - logit_second).astype(jnp.bfloat16)
    gate_second = jax.nn.sigmoid(logit_second - logit_first).astype(jnp.bfloat16)
    ranks = priority[0]
    earlier = (ranks[None, :] < ranks[:, None]).astype(jnp.bfloat16)
    before_first = jnp.dot(
        earlier, first_hot.astype(jnp.bfloat16), preferred_element_type=jnp.float32
    )
    before_second = jnp.dot(
        earlier, second_hot.astype(jnp.bfloat16), preferred_element_type=jnp.float32
    )
    first_load = jnp.sum(first_hot, axis=0)
    pos_first = jnp.sum(before_first * first_hot, axis=1).astype(jnp.int32)
    pos_second = jnp.sum((before_second + first_load[None, :]) * second_hot, axis=1).astype(
        jnp.int32
    )
    slot_first = jnp.where(pos_first < slot_cap, first * slot_cap + pos_first, -1)
    slot_second = jnp.where(pos_second < slot_cap, second * slot_cap + pos_second, -1)
    slot_grid = lax.broadcasted_iota(jnp.int32, (experts * slot_cap, group_rows), 0)
    dispatch = ((slot_grid == slot_first[None, :]) | (slot_grid == slot_second[None, :])).astype(
        jnp.bfloat16
    )
    outgoing = jnp.dot(dispatch, tokens, preferred_element_type=jnp.float32).astype(jnp.bfloat16)
    outgoing = outgoing.reshape(owner_count, column_count, slot_cap, width)
    arrived = send_rows(outgoing)
    expert_rows = arrived.reshape(experts * slot_cap, width)
    hidden = jax.nn.relu(jnp.dot(expert_rows, w_in[0], preferred_element_type=jnp.float32)).astype(
        jnp.bfloat16
    )
    produced = lax.dot_general(
        hidden, w_out[0], (((1,), (1,)), ((), ())), preferred_element_type=jnp.float32
    ).astype(jnp.bfloat16)
    returned = return_rows(produced.reshape(owner_count, column_count, slot_cap, width))
    returned = returned.reshape(experts * slot_cap, width)
    token_grid = lax.broadcasted_iota(jnp.int32, (group_rows, experts * slot_cap), 1)
    nothing = jnp.zeros((), jnp.bfloat16)
    combine = jnp.where(
        token_grid == slot_first[:, None], gate_first[:, None], nothing
    ) + jnp.where(token_grid == slot_second[:, None], gate_second[:, None], nothing)
    mixed = jnp.dot(combine, returned, preferred_element_type=jnp.float32).astype(jnp.bfloat16)
    prob_sum = jnp.sum(probs, axis=0)
    statistics = jnp.stack([prob_sum, first_load], axis=0)
    all_tokens = group_rows * owner_count * column_count
    totals = lax.psum(statistics, ("expert", "dp"))
    aux_loss = experts * jnp.sum(totals[0] / all_tokens * (totals[1] / all_tokens))
    return (mixed, aux_loss)


def solution(mesh):
    placed = (
        P(("expert", "dp"), None),
        P(("expert", "dp"), None),
        P(("expert", "dp"), None),
        P(),
        P(("expert", "dp"), None, None),
        P(("expert", "dp"), None, None),
    )
    return jax.shard_map(
        shards,
        mesh=mesh,
        in_specs=placed,
        out_specs=(P(("expert", "dp"), None), P()),
        check_vma=False,
    )
```
